32 devices in a mesh: groups: 2 (over x), expert: 16 (over z, y, core).
Axes of the slice: x: 2, y: 2, z: 4, core: 2. Of those that a mesh axis runs over, the one named last changes fastest.
Arguments:
- queries: bfloat16 [256, 4096], P(('groups', 'expert')), parts along dimension 0, may hold values from -150 to 150
- key_cache: bfloat16 [256, 64, 512], P(('groups', 'expert')), parts along dimension 0, may hold values from -7 to 7
- value_cache: bfloat16 [256, 64, 512], P(('groups', 'expert')), parts along dimension 0, may hold values from -6 to 6
- new_key: bfloat16 [256, 512], P(('groups', 'expert')), parts along dimension 0, may hold values from -6 to 6
- new_value: bfloat16 [256, 512], P(('groups', 'expert')), parts along dimension 0, may hold values from -6 to 6
- cache_lengths: int32 [256], P(('groups', 'expert')), parts along dimension 0, may hold values from 2 to 64, as said below
- hidden_in: bfloat16 [2048, 2048], P(('groups', 'expert')), parts along dimension 0, may hold values from -6 to 6
- norm_gain: bfloat16 [2048], replicated, may hold values from 0.5 to 1.5
- router_weight: bfloat16 [2048, 16], replicated, may hold values from -0.125 to 0.125
- expert_ids: int32 [2048, 8], P(('groups', 'expert')), parts along dimension 0, may hold values from 0 to 15, all different within a row; in each aligned block of 64 rows (0 to 63, 64 to 127, ...) at most 64 rows name the same one
- gate_train: bfloat16 [16, 2048, 768], P(None, 'expert'), may hold values from -0.125 to 0.125
- up_train: bfloat16 [16, 2048, 768], P(None, 'expert'), may hold values from -0.125 to 0.125
- down_train: bfloat16 [16, 768, 2048], P(None, 'expert'), may hold values from -0.21875 to 0.21875
Outputs:
- attended: bfloat16 [256, 4096], P(('groups', 'expert')), parts along dimension 0
- expert_mix: bfloat16 [2048, 2048], P(('groups', 'expert')), parts along dimension 0
The draws below stay inside these ranges and needn't reach their ends.
There are 2 independent parts, one for each index of `groups`. The reference program is written for one: setup_inputs(seed, part) draws one part's arguments, and reference() takes and returns one part's arrays. A program takes and returns all parts, laid end to end along the dimension named above; an argument that names none is the same for every part. Nothing has to cross between parts.
Inputs may be any that keep to these rules, and one draw needn't show every extreme that they name: `expert_ids`: each row names 8 different experts; within the rows of one device no expert is named more than 64 times. `cache_lengths`: the first sequence of each device's 8 has all 64 positions filled.
All inputs are finite; a program needn't handle non-finite values.
Results may differ from the reference program's by a relative error of at most 0.0074.
Values may be sent and summed in bfloat16 or wider, within the bound.
No kernel may reach another device: no remote copies, remote signals or barrier semaphores. Data moves between devices by JAX's collectives and lax.ppermute only.
A program may use at most 128 MiB of HBM per device.

```python
import math
import jax
import jax.numpy as jnp
import numpy as np
from jax import lax

D = 2048
FF = 768
HEADS = 32
KV_HEADS = 4
HEAD_DIM = 128
TOP = 8
TOK_DEV = 64
ATT_DEV = 8
CTX = 64
EXPERTS = 16
TOKENS = 1024
SEQS = 128
CAP = 64
N_EXPERT = 16


def cache_base(key):
    return jnp.clip(jax.random.normal(jax.random.fold_in(key, 7), (SEQS, CTX, KV_HEADS * HEAD_DIM), jnp.float32), -6.0, 6.0)


def draw_key_cache(key, part):
    values = cache_base(key)
    return values.astype(jnp.bfloat16)


def draw_queries(key, part):
    values = jnp.clip(jax.random.normal(jax.random.fold_in(key, 9), (SEQS, HEADS * HEAD_DIM), jnp.float32), -6.0, 6.0)
    return values.astype(jnp.bfloat16)


def draw_cache_lengths(key, part):
    lengths = jax.random.randint(jax.random.fold_in(key, 12), (SEQS,), 2, CTX + 1, jnp.int32)
    return lengths.at[::ATT_DEV].set(CTX)


def levels(rng, shape, shards, low, top_value):
    loudness, own = 1.0, jax.random.fold_in(rng, 6)
    for dim, blocks in shards:
        heights = jnp.exp(jax.random.uniform(jax.random.fold_in(own, dim), (blocks,), jnp.float32, low / len(shards), top_value / len(shards)))
        loudness = loudness * jnp.repeat(heights, shape[dim] // blocks).reshape([-1 if axis == dim else 1 for axis in range(len(shape))])
    return loudness


def shared_out(key, own, number, rows, amount, top, bound, slope):
    order = jax.random.permutation(key, amount)
    heavy_load, common = shares(amount, rows * top, bound, slope, True), shares(amount, rows * top, bound, slope, False)
    places = jnp.arange(amount)

    def named(sizes, offset_by):
        used = int((sizes > 0).sum())
        fixed = max(1, used // 4)
        moved = fixed + (places - fixed + offset_by * (used - fixed)) % max(1, amount - fixed)
        return jnp.zeros((amount,), jnp.int32).at[order[jnp.where(places < fixed, places, moved)]].set(jnp.asarray(sizes, jnp.int32))

    sizes = jnp.where(number % 4 == 0, named(heavy_load, number // 4), named(common, number - number // 4 - 1))
    mixed = jax.random.permutation(jax.random.fold_in(own, 3), amount)
    giver, taker = mixed[0:amount // 2 * 2:2], mixed[1:amount // 2 * 2:2]
    margin = jnp.minimum(sizes[giver] - 1, bound - sizes[taker]) // 2
    margin = jnp.where((giver == order[0]) | (taker == order[0]) | (sizes[taker] == 0), 0, jnp.maximum(margin, 0))
    moved = jax.random.randint(jax.random.fold_in(own, 4), (amount // 2,), 0, 1 << 20) % (margin + 1)
    sizes = sizes.at[giver].add(-moved).at[taker].add(moved)
    labels = jnp.searchsorted(jnp.cumsum(sizes), jnp.arange(rows * top), side="right").astype(jnp.int32)
    listing = labels.reshape(top, rows).T
    listing = listing[jax.random.permutation(jax.random.fold_in(own, 1), rows)]
    offset_by = jax.random.randint(jax.random.fold_in(own, 2), (rows, 1), 0, top)
    return jnp.take_along_axis(listing, (jnp.arange(top)[None, :] + offset_by) % top, axis=1)


def shares(amount, total, reach, slope, full):
    loads = [(1 << 20) // math.isqrt(rank ** slope) + 1 for rank in range(1, amount + 1)]
    largest = reach if full else min(reach, max(-(-total // amount), total * loads[0] // sum(loads)))
    least = 1 if total - largest >= amount - 1 else 0
    holding, spare = [largest] + [least] * (amount - 1), total - largest - least * (amount - 1)
    while spare > 0:
        movable = [i for i in range(1, amount) if holding[i] < largest] or [i for i in range(1, amount) if holding[i] < reach]
        whole, left = sum([loads[i] for i in movable]), spare
        for i in movable:
            addition = min(reach - holding[i], max(1, left * loads[i] // whole), spare)
            holding[i] = holding[i] + addition
            spare = spare - addition
    return np.array(holding)


def centred(key, dims, width, limit, cuts=(), kind=jnp.bfloat16):
    result = width * jax.random.normal(key, dims, jnp.float32)
    if cuts:
        result = result * levels(key, dims, cuts, -0.22, 0.18)
    return jnp.clip(result, -limit, limit).astype(kind)


def setup_inputs(seed: int = 0, part: int = 0) -> dict:
    keys = jax.random.split(jax.random.key(seed), 14)
    part_keys = jax.random.split(jax.random.fold_in(keys[13], part), 14)
    queries = draw_queries(jax.random.fold_in(jax.random.fold_in(keys[13], part), 71), part)
    key_cache = draw_key_cache(jax.random.fold_in(jax.random.fold_in(keys[13], part), 71), part)
    value_cache = centred(part_keys[2], (SEQS, CTX, KV_HEADS * HEAD_DIM), 1.0, 6.0, ((0, 16),))
    new_key = centred(part_keys[3], (SEQS, KV_HEADS * HEAD_DIM), 1.0, 6.0, ((0, 16),))
    new_value = centred(part_keys[4], (SEQS, KV_HEADS * HEAD_DIM), 1.0, 6.0, ((0, 16),))
    cache_lengths = draw_cache_lengths(jax.random.fold_in(jax.random.fold_in(keys[13], part), 71), part)
    hidden_in = centred(part_keys[6], (TOKENS, D), 1.0, 6.0, ((0, 16),))
    norm_gain = jnp.clip(1.0 + 0.1 * jax.random.normal(keys[7], (D,), jnp.float32), 0.5, 1.5).astype(jnp.bfloat16)
    router_weight = centred(keys[8], (D, EXPERTS), D ** -0.5, 0.125)
    expert_ids_keys = jax.random.split(jax.random.fold_in(part_keys[9], 1), TOKENS // TOK_DEV)
    expert_ids_turns = jax.random.permutation(jax.random.fold_in(part_keys[9], 3), TOKENS // TOK_DEV)
    expert_ids = jax.vmap(lambda own, number: shared_out(jax.random.fold_in(part_keys[9], 2), own, number, TOK_DEV, EXPERTS, TOP, CAP, 1))(expert_ids_keys, expert_ids_turns).reshape((TOKENS, TOP))
    gate_train = centred(keys[10], (EXPERTS, D, FF), D ** -0.5, 0.125, ((1, 16),))
    up_train = centred(keys[11], (EXPERTS, D, FF), D ** -0.5, 0.125, ((1, 16),))
    down_train = centred(keys[12], (EXPERTS, FF, D), FF ** -0.5, 0.21875, ((1, 16),))
    return dict(queries=queries, key_cache=key_cache, value_cache=value_cache, new_key=new_key, new_value=new_value, cache_lengths=cache_lengths, hidden_in=hidden_in, norm_gain=norm_gain, router_weight=router_weight, expert_ids=expert_ids, gate_train=gate_train, up_train=up_train, down_train=down_train)


EPSILON = 1e-06

def rms_normed(hidden_in, norm_gain):
    values = hidden_in.astype(jnp.float32)
    mean_square = lax.optimization_barrier(jnp.mean(values * values, axis=-1, keepdims=True))
    return (values * lax.rsqrt(mean_square + EPSILON) * norm_gain.astype(jnp.float32)).astype(jnp.bfloat16)

def attend(queries, key_cache, value_cache, new_key, new_value, cache_lengths):
    seq_count = queries.shape[0]
    group_size = HEADS // KV_HEADS
    query_blocks = queries.astype(jnp.float32).reshape(seq_count, KV_HEADS, group_size, HEAD_DIM)
    cached_keys = key_cache.astype(jnp.float32).reshape(seq_count, CTX, KV_HEADS, HEAD_DIM)
    cached_values = value_cache.astype(jnp.float32).reshape(seq_count, CTX, KV_HEADS, HEAD_DIM)
    fresh_keys = new_key.astype(jnp.float32).reshape(seq_count, KV_HEADS, HEAD_DIM)
    fresh_values = new_value.astype(jnp.float32).reshape(seq_count, KV_HEADS, HEAD_DIM)
    score_scale = 1.0 / math.sqrt(HEAD_DIM)
    scores = jnp.einsum('sgrd,scgd->sgrc', query_blocks, cached_keys) * score_scale
    own_score = jnp.einsum('sgrd,sgd->sgr', query_blocks, fresh_keys) * score_scale
    positions = jnp.arange(CTX, dtype=jnp.int32)
    visible = positions[None, :] < cache_lengths.astype(jnp.int32)[:, None]
    scores = jnp.where(visible[:, None, None, :], scores, -1e+30)
    largest = jnp.maximum(lax.optimization_barrier(jnp.max(scores, axis=-1)), own_score)
    cached_exp = jnp.exp(scores - largest[..., None])
    own_exp = jnp.exp(own_score - largest)
    prob_total = lax.optimization_barrier(jnp.sum(cached_exp, axis=-1)) + own_exp
    cached_prob = lax.optimization_barrier((cached_exp / prob_total[..., None]).astype(jnp.bfloat16)).astype(jnp.float32)
    own_prob = lax.optimization_barrier((own_exp / prob_total).astype(jnp.bfloat16)).astype(jnp.float32)
    context = jnp.einsum('sgrc,scgd->sgrd', cached_prob, cached_values)
    context = context + own_prob[..., None] * fresh_values[:, :, None, :]
    return context.reshape(seq_count, HEADS * HEAD_DIM).astype(jnp.bfloat16)

def expert_block(operands):
    token_rows, gate_weight, up_weight, down_weight = operands
    gate_proj = jnp.dot(token_rows, gate_weight, preferred_element_type=jnp.float32)
    up_proj = jnp.dot(token_rows, up_weight, preferred_element_type=jnp.float32)
    hidden_units = (jax.nn.silu(gate_proj) * up_proj).astype(jnp.bfloat16)
    return jnp.dot(hidden_units, down_weight, preferred_element_type=jnp.float32).astype(jnp.bfloat16)

def mix_experts(hidden_in, norm_gain, router_weight, expert_ids, gate_train, up_train, down_train):
    normed = rms_normed(hidden_in, norm_gain)
    logits = jnp.dot(normed, router_weight, preferred_element_type=jnp.float32)
    expert_range = jnp.arange(EXPERTS, dtype=jnp.int32)
    picked = expert_ids.astype(jnp.int32)[:, :, None] == expert_range[None, None, :]
    chosen = lax.optimization_barrier(jnp.sum(jnp.where(picked, logits[:, None, :], 0.0), axis=-1))
    mixing = jax.nn.softmax(chosen, axis=-1)
    onehot_int = picked.astype(jnp.int32).reshape(N_EXPERT, TOK_DEV * TOP, EXPERTS)
    rank_values = lax.optimization_barrier(jnp.sum((jnp.cumsum(onehot_int, axis=1).astype(jnp.int32) - 1) * onehot_int, axis=-1)).astype(jnp.int32)
    sources = jnp.arange(N_EXPERT, dtype=jnp.int32)[:, None]
    slot_index = (sources * CAP + rank_values).reshape(-1).astype(jnp.int32)
    flat_ids = expert_ids.reshape(-1).astype(jnp.int32)
    repeated = jnp.repeat(normed, TOP, axis=0)
    buffers = jnp.zeros((EXPERTS, N_EXPERT * CAP, D), jnp.bfloat16).at[flat_ids, slot_index].set(repeated)
    outputs = lax.map(expert_block, (buffers, gate_train, up_train, down_train))
    returned = outputs[flat_ids, slot_index].astype(jnp.float32).reshape(TOKENS, TOP, D)
    return lax.optimization_barrier(jnp.sum(mixing[:, :, None] * returned, axis=1)).astype(jnp.bfloat16)

def reference(queries, key_cache, value_cache, new_key, new_value, cache_lengths, hidden_in, norm_gain, router_weight, expert_ids, gate_train, up_train, down_train):
    attended = attend(queries, key_cache, value_cache, new_key, new_value, cache_lengths)
    expert_mix = mix_experts(hidden_in, norm_gain, router_weight, expert_ids, gate_train, up_train, down_train)
    return (attended, expert_mix)
```

```python
import math

import jax
import jax.numpy as jnp
from jax import lax
from jax.sharding import PartitionSpec as P


HEADS = 32
KV_HEADS = 4
HEAD_DIM = 128
CTX = 64


EPSILON = 1e-06
PIECES = 2


def rms_normed(hidden_in, norm_gain):
    values = hidden_in.astype(jnp.float32)
    mean_square = jnp.mean(values * values, axis=-1, keepdims=True)
    return (values * lax.rsqrt(mean_square + EPSILON) * norm_gain.astype(jnp.float32)).astype(
        jnp.bfloat16
    )


def attend(queries, key_cache, value_cache, new_key, new_value, cache_lengths):
    seq_count = queries.shape[0]
    group_size = HEADS // KV_HEADS
    query_blocks = queries.reshape(seq_count, KV_HEADS, group_size, HEAD_DIM)
    cached_keys = key_cache.reshape(seq_count, CTX, KV_HEADS, HEAD_DIM)
    cached_values = value_cache.reshape(seq_count, CTX, KV_HEADS, HEAD_DIM)
    fresh_keys = new_key.reshape(seq_count, KV_HEADS, HEAD_DIM)
    fresh_values = new_value.astype(jnp.float32).reshape(seq_count, KV_HEADS, HEAD_DIM)
    score_scale = 1.0 / math.sqrt(HEAD_DIM)
    scores = (
        jnp.einsum("sgrd,scgd->sgrc", query_blocks, cached_keys, preferred_element_type=jnp.float32)
        * score_scale
    )
    own_score = (
        jnp.einsum("sgrd,sgd->sgr", query_blocks, fresh_keys, preferred_element_type=jnp.float32)
        * score_scale
    )
    positions = jnp.arange(CTX, dtype=jnp.int32)
    visible = positions[None, :] < cache_lengths[:, None]
    scores = jnp.where(visible[:, None, None, :], scores, -1e30)
    largest = jnp.maximum(jnp.max(scores, axis=-1), own_score)
    cached_exp = jnp.exp(scores - largest[..., None])
    own_exp = jnp.exp(own_score - largest)
    prob_total = jnp.sum(cached_exp, axis=-1) + own_exp
    cached_prob = (cached_exp / prob_total[..., None]).astype(jnp.bfloat16)
    own_prob = (own_exp / prob_total).astype(jnp.bfloat16).astype(jnp.float32)
    context = jnp.einsum(
        "sgrc,scgd->sgrd", cached_prob, cached_values, preferred_element_type=jnp.float32
    )
    context = context + own_prob[..., None] * fresh_values[:, :, None, :]
    return context.reshape(seq_count, HEADS * HEAD_DIM).astype(jnp.bfloat16)


def shifted(value, step):
    count = lax.axis_size("groups")
    return lax.ppermute(value, "groups", [(i, (i + step) % count) for i in range(count)])


def moved(train, part, parts, piece=0, pieces=1):
    width = train.shape[2] // (parts * pieces)
    own = lax.dynamic_slice_in_dim(train, (part * pieces + piece) * width, width, axis=2)
    block = lax.all_to_all(own, "expert", split_axis=0, concat_axis=0, tiled=True)
    return block.reshape(-1, width)


def summed(partial):
    count = lax.axis_size("expert")
    index = lax.axis_index("expert")
    if count & (count - 1):
        return lax.psum_scatter(
            partial.astype(jnp.bfloat16), "expert", scatter_dimension=0, tiled=True
        )
    total_bits = count.bit_length() - 1
    low_bits = min(2, total_bits)
    order = list(range(low_bits)) + list(range(total_bits - 1, low_bits - 1, -1))
    rows, width = partial.shape
    left = sorted(order)
    kept = partial.reshape((2,) * total_bits + (rows // count, width))
    for bit in order:
        axis = len(left) - 1 - left.index(bit)
        side = (index >> bit) & 1
        out = lax.dynamic_index_in_dim(kept, 1 - side, axis, keepdims=False)
        own = lax.dynamic_index_in_dim(kept, side, axis, keepdims=False)
        pairs = [(i, i ^ (1 << bit)) for i in range(count)]
        came = lax.ppermute(out.astype(jnp.bfloat16), "expert", pairs)
        kept = own.astype(jnp.float32) + came.astype(jnp.float32)
        left.remove(bit)
    return kept.astype(jnp.bfloat16)


def local(
    queries,
    key_cache,
    value_cache,
    new_key,
    new_value,
    cache_lengths,
    hidden_in,
    norm_gain,
    router_weight,
    expert_ids,
    gate_train,
    up_train,
    down_train,
):
    parts = lax.axis_size("groups")
    part = lax.axis_index("groups")
    own_index = lax.axis_index("expert")
    tok_count, width = hidden_in.shape
    expert_count = router_weight.shape[1]

    normed = rms_normed(hidden_in, norm_gain)
    logits = jnp.dot(normed, router_weight, preferred_element_type=jnp.float32)
    expert_range = jnp.arange(expert_count, dtype=jnp.int32)
    picked = jnp.any(expert_ids[:, :, None] == expert_range[None, None, :], axis=1)
    largest = jnp.max(jnp.where(picked, logits, -jnp.inf), axis=-1, keepdims=True)
    raised = jnp.where(picked, jnp.exp(jnp.where(picked, logits - largest, 0.0)), 0.0)
    mixing = raised / jnp.sum(raised, axis=-1, keepdims=True)
    high = lax.reduce_precision(mixing, 8, 7)
    low = mixing - high
    spare = -(2 * expert_count) % 128
    sent = jnp.concatenate(
        (
            normed,
            high.astype(jnp.bfloat16),
            low.astype(jnp.bfloat16),
            jnp.zeros((tok_count, spare), jnp.bfloat16),
        ),
        axis=1,
    )
    everything = lax.all_gather(sent, "expert", axis=0, tiled=True)

    gate_own = moved(gate_train, part, parts)
    up_own = moved(up_train, part, parts)
    down_pieces = [moved(down_train, part, parts, i, PIECES) for i in range(PIECES)]

    attended = attend(queries, key_cache, value_cache, new_key, new_value, cache_lengths)

    all_rows = everything[:, :width]
    tail = everything[:, width:].astype(jnp.float32)
    lane = jnp.arange(tail.shape[1], dtype=jnp.int32)
    mine = (lane == own_index) | (lane == own_index + expert_count)
    weight = jnp.sum(jnp.where(mine[None, :], tail, 0.0), axis=1, keepdims=True)

    unit_width = gate_own.shape[1]
    hidden_units = jnp.zeros((all_rows.shape[0], unit_width * parts), jnp.bfloat16)
    for step in range(parts):
        gate_weight = gate_own if step == 0 else shifted(gate_own, step)
        up_weight = up_own if step == 0 else shifted(up_own, step)
        gate_proj = jnp.dot(all_rows, gate_weight, preferred_element_type=jnp.float32)
        up_proj = jnp.dot(all_rows, up_weight, preferred_element_type=jnp.float32)
        units = (jax.nn.silu(gate_proj) * up_proj).astype(jnp.bfloat16)
        place = (part + parts - step) % parts
        hidden_units = lax.dynamic_update_slice_in_dim(
            hidden_units, units, place * unit_width, axis=1
        )

    out_width = down_pieces[0].shape[1]
    mixed_out = jnp.zeros((tok_count, width), jnp.bfloat16)
    for step in range(parts):
        for number, down_own in enumerate(down_pieces):
            down_weight = down_own if step == 0 else shifted(down_own, step)
            expert_out = jnp.dot(hidden_units, down_weight, preferred_element_type=jnp.float32)
            reduced = summed((weight * expert_out).astype(jnp.bfloat16))
            place = ((part + parts - step) % parts) * PIECES + number
            mixed_out = lax.dynamic_update_slice_in_dim(
                mixed_out, reduced, place * out_width, axis=1
            )
    return (attended, mixed_out)


def solution(mesh):
    placed = (
        P(("groups", "expert"), None),
        P(("groups", "expert"), None, None),
        P(("groups", "expert"), None, None),
        P(("groups", "expert"), None),
        P(("groups", "expert"), None),
        P(("groups", "expert")),
        P(("groups", "expert"), None),
        P(),
        P(),
        P(("groups", "expert"), None),
        P(None, "expert", None),
        P(None, "expert", None),
        P(None, "expert", None),
    )

    return jax.shard_map(
        local,
        mesh=mesh,
        in_specs=placed,
        out_specs=(P(("groups", "expert"), None), P(("groups", "expert"), None)),
        check_vma=False,
    )
```

```python
import math

import jax
import jax.numpy as jnp
from jax import lax
from jax.sharding import PartitionSpec as P


HEADS = 32
KV_HEADS = 4
HEAD_DIM = 128
CTX = 64


EPSILON = 1e-06
PIECES = 2
EARLY = 1
GROUPED = True


def rms_normed(hidden_in, norm_gain):
    values = hidden_in.astype(jnp.float32)
    mean_square = jnp.mean(values * values, axis=-1, keepdims=True)
    return (values * lax.rsqrt(mean_square + EPSILON) * norm_gain.astype(jnp.float32)).astype(
        jnp.bfloat16
    )


def attend(queries, key_cache, value_cache, new_key, new_value, cache_lengths):
    seq_count = queries.shape[0]
    group_size = HEADS // KV_HEADS
    query_blocks = queries.reshape(seq_count, KV_HEADS, group_size, HEAD_DIM)
    cached_keys = key_cache.reshape(seq_count, CTX, KV_HEADS, HEAD_DIM)
    cached_values = value_cache.reshape(seq_count, CTX, KV_HEADS, HEAD_DIM)
    fresh_keys = new_key.reshape(seq_count, KV_HEADS, HEAD_DIM)
    fresh_values = new_value.astype(jnp.float32).reshape(seq_count, KV_HEADS, HEAD_DIM)
    score_scale = 1.0 / math.sqrt(HEAD_DIM)
    scores = (
        jnp.einsum("sgrd,scgd->sgrc", query_blocks, cached_keys, preferred_element_type=jnp.float32)
        * score_scale
    )
    own_score = (
        jnp.einsum("sgrd,sgd->sgr", query_blocks, fresh_keys, preferred_element_type=jnp.float32)
        * score_scale
    )
    positions = jnp.arange(CTX, dtype=jnp.int32)
    visible = positions[None, :] < cache_lengths[:, None]
    scores = jnp.where(visible[:, None, None, :], scores, -1e30)
    largest = jnp.maximum(jnp.max(scores, axis=-1), own_score)
    cached_exp = jnp.exp(scores - largest[..., None])
    own_exp = jnp.exp(own_score - largest)
    prob_total = jnp.sum(cached_exp, axis=-1) + own_exp
    cached_prob = (cached_exp / prob_total[..., None]).astype(jnp.bfloat16)
    own_prob = (own_exp / prob_total).astype(jnp.bfloat16).astype(jnp.float32)
    context = jnp.einsum(
        "sgrc,scgd->sgrd", cached_prob, cached_values, preferred_element_type=jnp.float32
    )
    context = context + own_prob[..., None] * fresh_values[:, :, None, :]
    return context.reshape(seq_count, HEADS * HEAD_DIM).astype(jnp.bfloat16)


def shifted(value, step):
    count = lax.axis_size("groups")
    return lax.ppermute(value, "groups", [(i, (i + step) % count) for i in range(count)])


def moved(train, part, parts, piece=0, pieces=1):
    width = train.shape[2] // (parts * pieces)
    own = lax.dynamic_slice_in_dim(train, (part * pieces + piece) * width, width, axis=2)
    block = lax.all_to_all(own, "expert", split_axis=0, concat_axis=0, tiled=True)
    return block.reshape(-1, width)


def stage_bits(count):
    if count & (count - 1):
        return [None]
    total_bits = count.bit_length() - 1
    low_bits = min(2, total_bits)
    order = [(bit,) for bit in range(low_bits)]
    high = list(range(total_bits - 1, low_bits - 1, -1))
    while high:
        order.append(tuple(high[:2]))
        high = high[2:]
    return order


def staged(partial, count):
    rows, width = partial.shape
    if count & (count - 1):
        return partial
    return partial.reshape((2,) * (count.bit_length() - 1) + (rows // count, width))


def halved(kept, number):
    count = lax.axis_size("expert")
    order = stage_bits(count)
    bits = order[number]
    if bits is None:
        return lax.psum_scatter(kept, "expert", scatter_dimension=0, tiled=True)
    left = sorted(sum(order[number:], ()))
    index = lax.axis_index("expert")

    def picked(flips):
        part = kept
        remaining = list(left)
        for bit in bits:
            axis = len(remaining) - 1 - remaining.index(bit)
            side = (index >> bit) & 1
            side = 1 - side if bit in flips else side
            part = lax.dynamic_index_in_dim(part, side, axis, keepdims=False)
            remaining.remove(bit)
        return part

    choices = [()]
    for bit in bits:
        choices = choices + [flips + (bit,) for flips in choices]
    total = picked(()).astype(jnp.float32)
    for flips in choices[1:]:
        mask = sum(1 << bit for bit in flips)
        pairs = [(i, i ^ mask) for i in range(count)]
        came = lax.ppermute(picked(flips).astype(jnp.bfloat16), "expert", pairs)
        total = total + came.astype(jnp.float32)
    return total


def local(
    queries,
    key_cache,
    value_cache,
    new_key,
    new_value,
    cache_lengths,
    hidden_in,
    norm_gain,
    router_weight,
    expert_ids,
    gate_train,
    up_train,
    down_train,
):
    parts = lax.axis_size("groups")
    part = lax.axis_index("groups")
    own_index = lax.axis_index("expert")
    tok_count, width = hidden_in.shape
    expert_count = router_weight.shape[1]

    normed = rms_normed(hidden_in, norm_gain)
    logits = jnp.dot(normed, router_weight, preferred_element_type=jnp.float32)
    expert_range = jnp.arange(expert_count, dtype=jnp.int32)
    picked = jnp.any(expert_ids[:, :, None] == expert_range[None, None, :], axis=1)
    largest = jnp.max(jnp.where(picked, logits, -jnp.inf), axis=-1, keepdims=True)
    raised = jnp.where(picked, jnp.exp(jnp.where(picked, logits - largest, 0.0)), 0.0)
    mixing = raised / jnp.sum(raised, axis=-1, keepdims=True)
    high = lax.reduce_precision(mixing, 8, 7)
    low = mixing - high
    spare = -(2 * expert_count) % 128
    sent = jnp.concatenate(
        (
            normed,
            high.astype(jnp.bfloat16),
            low.astype(jnp.bfloat16),
            jnp.zeros((tok_count, spare), jnp.bfloat16),
        ),
        axis=1,
    )
    everything = lax.all_gather(sent, "expert", axis=0, tiled=True)

    gate_own = moved(gate_train, part, parts)
    up_own = moved(up_train, part, parts)
    down_pieces = [moved(down_train, part, parts, i, PIECES) for i in range(PIECES)]

    attended = attend(queries, key_cache, value_cache, new_key, new_value, cache_lengths)

    all_rows = everything[:, :width]
    tail = everything[:, width:].astype(jnp.float32)
    lane = jnp.arange(tail.shape[1], dtype=jnp.int32)
    mine = (lane == own_index) | (lane == own_index + expert_count)
    weight = jnp.sum(jnp.where(mine[None, :], tail, 0.0), axis=1, keepdims=True)

    unit_width = gate_own.shape[1]
    hidden_units = jnp.zeros((all_rows.shape[0], unit_width * parts), jnp.bfloat16)
    for step in range(parts):
        gate_weight = gate_own if step == 0 else shifted(gate_own, step)
        up_weight = up_own if step == 0 else shifted(up_own, step)
        gate_proj = jnp.dot(all_rows, gate_weight, preferred_element_type=jnp.float32)
        up_proj = jnp.dot(all_rows, up_weight, preferred_element_type=jnp.float32)
        units = (jax.nn.silu(gate_proj) * up_proj).astype(jnp.bfloat16)
        place = (part + parts - step) % parts
        hidden_units = lax.dynamic_update_slice_in_dim(
            hidden_units, units, place * unit_width, axis=1
        )

    def scaled(down_weight):
        expert_out = jnp.dot(hidden_units, down_weight, preferred_element_type=jnp.float32)
        return (weight * expert_out).astype(jnp.bfloat16)

    out_width = down_pieces[0].shape[1]
    keys = [(step, number) for number in range(PIECES) for step in range(parts)]
    weights = [
        down_pieces[number] if step == 0 else shifted(down_pieces[number], step)
        for step, number in keys
    ]
    device_count = lax.axis_size("expert")
    stages = len(stage_bits(device_count))
    if GROUPED:
        grouped = [[0], list(range(1, len(keys) - 1)), [len(keys) - 1]]
    else:
        grouped = [[i] for i in range(len(keys))]
    joined = [
        weights[group[0]]
        if len(group) == 1
        else jnp.concatenate([weights[i] for i in group], axis=1)
        for group in grouped
    ]
    chains = []
    reach = min(EARLY, stages)
    for number, weight_ in enumerate(joined):
        if number and reach:
            chains[-1], weight_ = lax.optimization_barrier((chains[-1], weight_))
        if number:
            for stage in range(reach, stages):
                chains[-1] = halved(chains[-1], stage)
        chain = staged(scaled(weight_), device_count)
        for stage in range(reach):
            chain = halved(chain, stage)
        chains.append(chain)
    for stage in range(reach, stages):
        chains[-1] = halved(chains[-1], stage)
    reduced = jnp.concatenate(chains, axis=1).astype(jnp.bfloat16)
    mixed_out = jnp.zeros((tok_count, width), jnp.bfloat16)
    for place_, (step, number) in enumerate(keys):
        place = ((part + parts - step) % parts) * PIECES + number
        block = lax.slice_in_dim(reduced, place_ * out_width, (place_ + 1) * out_width, axis=1)
        mixed_out = lax.dynamic_update_slice_in_dim(
            mixed_out, block, place * out_width, axis=1
        )
    return (attended, mixed_out)


def solution(mesh):
    placed = (
        P(("groups", "expert"), None),
        P(("groups", "expert"), None, None),
        P(("groups", "expert"), None, None),
        P(("groups", "expert"), None),
        P(("groups", "expert"), None),
        P(("groups", "expert")),
        P(("groups", "expert"), None),
        P(),
        P(),
        P(("groups", "expert"), None),
        P(None, "expert", None),
        P(None, "expert", None),
        P(None, "expert", None),
    )

    return jax.shard_map(
        local,
        mesh=mesh,
        in_specs=placed,
        out_specs=(P(("groups", "expert"), None), P(("groups", "expert"), None)),
        check_vma=False,
    )
```
